32 devices in a mesh: span: 8 (over y, x, core), tok: 4 (over z).
Axes of the slice: x: 2, y: 2, z: 4, core: 2. Of those that a mesh axis runs over, the one named last changes fastest.
Arguments:
- queries: bfloat16 [8, 256, 3072], P('span', 'tok'), may hold values from -9 to 9
- keys: bfloat16 [8, 256, 3072], P('span', 'tok'), may hold values from -9 to 9
- values: bfloat16 [8, 256, 3072], P('span', 'tok'), may hold values from -6 to 6
- levels: int32 [8], P('span'), may hold values from 0 to 15
- retiring: int32 [1], replicated, may hold values from 0 to 7
- block_mask: int32 [8, 8], P('span'), may hold values 0 or 1
- gates: float32 [16, 3072], replicated, may hold values from 0.5 to 2
Outputs:
- attended: bfloat16 [8, 256, 3072], P('span', 'tok')
The draws below stay inside these ranges and needn't reach their ends.
All inputs are finite; a program needn't handle non-finite values. No bound on the sum of `block_mask` on one device may be relied on, other than what follows from the above.
Results may differ from the reference program's by a relative error of at most 0.0085.
Values may be sent and summed in bfloat16 or wider, within the bound.
A program may use at most 128 MiB of HBM per device.

```python
import math
import jax
import jax.numpy as jnp
from jax import lax

HEADS = 24
HEAD_DIM = 128
LEVELS = 16
FEAT = 3072
SPANS = 8
CTOK = 256


def base_draw(key, salt):
    base = jax.random.truncated_normal(jax.random.fold_in(key, salt), -4.0, 4.0, (SPANS, CTOK, HEADS * HEAD_DIM), jnp.float32)
    return base


def draw_queries(key, part):
    base = base_draw(key, 1)
    return base.astype(jnp.bfloat16)


def draw_keys(key, part):
    base = base_draw(key, 2)
    return base.astype(jnp.bfloat16)


def place_ends(values, rng, low, high):
    index_at = [jax.random.randint(jax.random.fold_in(rng, axis), (), 0, length) for axis, length in enumerate(values.shape)]
    widest = values.shape.index(max(values.shape))
    beside = index_at[:widest] + [(index_at[widest] + 1) % values.shape[widest]] + index_at[widest + 1:]
    return values.at[tuple(index_at)].set(low).at[tuple(beside)].set(high)


def block_scale(stream_key, shape, cuts, low, high):
    factor_of = 1.0
    for axis_at, blocks in cuts:
        draws = jax.random.uniform(jax.random.fold_in(jax.random.fold_in(stream_key, 6), axis_at), (blocks,), jnp.float32, low / len(cuts), high / len(cuts))
        factor_of = factor_of * jnp.repeat(jnp.exp(draws), shape[axis_at] // blocks).reshape((-1,) + (1,) * (len(shape) - 1 - axis_at))
    return factor_of


def centred(stream_key, dims, scale, bound, shards=(), kind=jnp.bfloat16):
    entries = scale * jax.random.normal(stream_key, dims, jnp.float32)
    if shards:
        entries = entries * block_scale(stream_key, dims, shards, -0.22, 0.18)
    return jnp.clip(entries, -bound, bound).astype(kind)


def setup_inputs(seed: int = 0) -> dict:
    seeds = jax.random.split(jax.random.key(seed), 8)
    queries = draw_queries(jax.random.fold_in(seeds[7], 71), 0)
    keys = draw_keys(jax.random.fold_in(seeds[7], 71), 0)
    values = centred(seeds[2], (SPANS, CTOK, FEAT), 1.0, 6.0, ((0, 8), (1, 4)))
    levels = place_ends(jax.random.randint(seeds[3], (SPANS,), 0, LEVELS), jax.random.fold_in(seeds[3], 1), 0, LEVELS - 1).astype(jnp.int32)
    retiring = jax.random.randint(seeds[4], (1,), 0, SPANS).astype(jnp.int32)
    block_mask = place_ends((jax.random.randint(seeds[5], (SPANS, SPANS), 0, 4) < 3).astype(jnp.int32), jax.random.fold_in(seeds[5], 1), 0, 1)
    gates = jnp.clip(jnp.exp(jax.random.uniform(seeds[6], (LEVELS, FEAT), jnp.float32, math.log(0.5), math.log(2.0))), 0.5, 2.0)
    return {"queries": queries, "keys": keys, "values": values, "levels": levels, "retiring": retiring, "block_mask": block_mask, "gates": gates}


def reference(queries, keys, values, levels, retiring, block_mask, gates):
    spans = queries.shape[0]
    ctok = queries.shape[1]
    slots = jnp.arange(spans, dtype=jnp.int32)
    order = (slots - retiring[0]) % spans
    allowed = (slots[:, None] == slots[None, :]) | ((block_mask == 1) & (order[None, :] < order[:, None]))
    all_keys = keys.reshape(spans * ctok, HEADS, HEAD_DIM)
    all_values = values.reshape(spans * ctok, HEADS, HEAD_DIM)
    scale = jnp.float32(HEAD_DIM ** -0.5)

    def per_span(slot):
        query = queries[slot].reshape(ctok, HEADS, HEAD_DIM)
        keep = jnp.repeat(allowed[slot], ctok)

        def per_head(head):
            score = jnp.dot(query[:, head], all_keys[:, head].T, preferred_element_type=jnp.float32) * scale
            score = jnp.where(keep[None, :], score, -jnp.inf)
            weight = jnp.exp(score - jnp.max(score, axis=-1, keepdims=True))
            total = jnp.sum(weight, axis=-1)
            mixed = jnp.dot(weight.astype(jnp.bfloat16), all_values[:, head], preferred_element_type=jnp.float32)
            return mixed / total[:, None]

        mixed = lax.map(per_head, jnp.arange(HEADS, dtype=jnp.int32))
        mixed = jnp.transpose(mixed, (1, 0, 2)).reshape(ctok, HEADS * HEAD_DIM)
        return (mixed * gates[levels[slot]][None, :]).astype(jnp.bfloat16)

    return lax.map(per_span, slots)
```

```python
import functools

import jax
import jax.numpy as jnp
from jax import lax
from jax.experimental import pallas as pl
from jax.experimental.pallas import tpu as pltpu
from jax.sharding import PartitionSpec as P

HEADS = 24
HEAD_DIM = 128
QUERY_BLOCK = 256
UNROLLED_KEYS = 2048


def ORDER(hpd):
    return [(kind, h) for h in range(hpd) for kind in ("kv", "q")]


def WAITS(toks):
    return range(1, toks)


def kernel(dims, q_ref, k_ref, v_ref, mask_ref, level_ref, retiring_ref, gates_ref, out_ref,
           qbuf, kbuf, vbuf, maskb, levelb, retb, gateb, mbuf, sbuf, obuf, total,
           sent, got, got_q, meta_sem, fwd_sent, fwd_got, core_sent, core_got, out_sent, out_got):
    spans, toks, g, hpd, rows = dims
    chips = spans // 2
    groups = chips // g
    ctok = rows * toks
    d = HEAD_DIM
    s = lax.axis_index("span")
    t = lax.axis_index("tok")
    c = lax.rem(s, 2)
    p = lax.div(s, 2)
    j = lax.rem(p, g)
    hi = lax.div(p, g)
    own = hi * g
    other = 1 - c

    def span_of(hi_, j_, c_):
        return (hi_ * g + j_) * 2 + c_

    partners = [(dt, dj) for dt in range(toks) for dj in range(g) if (dt, dj) != (0, 0)]
    partners.sort(key=lambda a: a[0])

    def shift_tok(by):
        if toks & (toks - 1) == 0:
            low = 0
            bit = 1
            while bit < toks:
                mine_bit = lax.rem(lax.div(t, bit), 2)
                low = low + bit * (1 - mine_bit if by & bit else mine_bit)
                bit *= 2
            return low
        return lax.rem(t + by, toks)

    def partner(dt, dj):
        return shift_tok(dt), lax.rem(j + dj, g)

    barrier = pltpu.get_barrier_semaphore()
    count = 0
    for dt, dj in partners:
        t2, j2 = partner(dt, dj)
        pl.semaphore_signal(barrier, inc=1, device_id=(span_of(hi, j2, c), t2),
                            device_id_type=pl.DeviceIdType.MESH)
        count += 1
    for dh in range(1, groups):
        pl.semaphore_signal(barrier, inc=1, device_id=(span_of(lax.rem(hi + dh, groups), j, c), t),
                            device_id_type=pl.DeviceIdType.MESH)
        count += 1
    pl.semaphore_signal(barrier, inc=1, device_id=(span_of(hi, j, other), t),
                        device_id_type=pl.DeviceIdType.MESH)
    pl.semaphore_wait(barrier, count + 1)

    def cols(t_, j_, h):
        return pl.ds(pl.multiple_of(((t_ * g + j_) * hpd + h) * d, d), d)

    my_rows = pl.ds(pl.multiple_of(t * rows, rows), rows)

    near = [a for a in partners if a[0] == 0]
    far = [a for a in partners if a[0] != 0]

    def arrays(kind, h):
        if kind == "q":
            return ((q_ref, qbuf.at[h, j, my_rows]),), got_q.at[h]
        return ((k_ref, kbuf.at[h, c, p, my_rows]), (v_ref, vbuf.at[h, c, p, my_rows])), got.at[h, t]

    def issue(kind, h, which):
        pairs, arrive = arrays(kind, h)
        for dt, dj in which:
            t2, j2 = partner(dt, dj)
            for src, dst in pairs:
                pltpu.make_async_remote_copy(
                    src.at[:, cols(t2, j2, h)], dst, sent, arrive,
                    device_id=(span_of(hi, j2, c), t2), device_id_type=pl.DeviceIdType.MESH).start()

    def keep(kind, h):
        pairs, arrive = arrays(kind, h)
        for src, dst in pairs:
            pltpu.make_async_copy(src.at[:, cols(t, j, h)], dst, arrive).start()

    for h in range(hpd):
        keep("kv", h)
        issue("kv", h, near)
    for kind, h in (("kv", 0), ("q", 0))[:2 * hpd - 1]:
        issue(kind, h, far)
    for h in range(hpd):
        keep("q", h)
        issue("q", h, near)

    def wait_bytes(ref, sem):
        pltpu.make_async_copy(ref, ref, sem).wait()

    mine = pl.ds(pl.multiple_of((t * g + j) * hpd * d, d), hpd * d)
    pltpu.make_async_copy(retiring_ref, retb, meta_sem.at[2]).start()
    pltpu.make_async_copy(gates_ref.at[:, mine], gateb, meta_sem.at[3]).start()
    for n, (src, dst) in enumerate(((mask_ref, maskb.at[j]), (level_ref, levelb.at[j]))):
        pltpu.make_async_copy(src, dst, meta_sem.at[n]).start()
        for dj in range(1, g):
            t2, j2 = partner(0, dj)
            pltpu.make_async_remote_copy(
                src, dst, meta_sem.at[4 + n], meta_sem.at[n],
                device_id=(span_of(hi, j2, c), t2), device_id_type=pl.DeviceIdType.MESH).start()
    wait_bytes(retb, meta_sem.at[2])
    wait_bytes(gateb, meta_sem.at[3])
    wait_bytes(maskb, meta_sem.at[0])
    wait_bytes(levelb, meta_sem.at[1])
    lane = lax.broadcasted_iota(jnp.int32, (1, spans), 1)
    level_at = lax.broadcasted_iota(jnp.int32, gateb.shape, 0)

    def age(slot):
        return lax.rem(slot - retb[...] + spans, spans)

    for i in range(g):
        slot = span_of(hi, i, c)
        see = (lane == slot) | ((maskb[i] == 1) & (age(lane) < age(slot)))
        mbuf[i, 1:2, 0:spans] = jnp.where(see, 1.0, 0.0)
        mbuf[i, 0:1] = jnp.sum(jnp.where(level_at == levelb[i], gateb[...], 0.0), axis=0, keepdims=True)
    c2 = jnp.float32(HEAD_DIM ** -0.5 * 1.4426950408889634)
    unrolled = 2 * chips * ctok <= UNROLLED_KEYS
    block = min(QUERY_BLOCK, ctok)

    def loop(count, body, carry):
        if unrolled:
            for n in range(count):
                carry = body(n, carry)
            return carry
        return lax.fori_loop(0, count, body, carry)

    def seen(i, half, chip):
        flags = mbuf[i, 1:2, 0:spans]
        lane = lax.broadcasted_iota(jnp.int32, flags.shape, 1)
        hit = lane == chip * 2 + half
        return jnp.sum(jnp.where(hit, flags, 0.0), axis=1, keepdims=True) > 0.5

    def scores(h, i, at, half, slot0, top):
        query = qbuf[h, i, at]

        def body(chip, top):
            score = lax.dot_general(kbuf[h, half, chip], query, (((1,), (1,)), ((), ())),
                                    preferred_element_type=jnp.float32)
            sbuf[slot0 + chip] = score
            best = jnp.max(score, axis=0, keepdims=True)
            return jnp.maximum(top, jnp.where(seen(i, half, chip), best, -1e30))

        return loop(chips, body, top)

    def mix(h, i, half, slot0, shift, carry):
        def body(chip, carry):
            acc, norm = carry
            minus = jnp.where(seen(i, half, chip), shift, 1e30)
            weight = jnp.exp2(sbuf[slot0 + chip] * c2 - minus)
            norm = norm + jnp.sum(weight, axis=0, keepdims=True)
            acc = acc + lax.dot_general(vbuf[h, half, chip], weight.astype(jnp.bfloat16),
                                        (((0,), (0,)), ((), ())), preferred_element_type=jnp.float32)
            return acc, norm

        return loop(chips, body, carry)

    def unit(h, i, b):
        at = pl.ds(b * block, block)
        top = jnp.full((1, block), -1e30, jnp.float32)
        top = scores(h, i, at, c, 0, top)
        top = scores(h, i, at, other, chips, top)
        shift = top * c2
        carry = (jnp.zeros((d, block), jnp.float32), jnp.zeros((1, block), jnp.float32))
        carry = mix(h, i, c, 0, shift, carry)
        acc, norm = mix(h, i, other, chips, shift, carry)
        mixed = (acc / norm).T
        gate = mbuf[i, 0:1, pl.ds(pl.multiple_of(h * d, d), d)]
        obuf[h, i, at] = (mixed * gate).astype(jnp.bfloat16)

    def relay(h, t2):
        rows2 = pl.ds(pl.multiple_of(t2 * rows, rows), rows)
        wait_bytes(total.at[pl.ds(0, 2 * g * rows)], got.at[h, t2])
        for dh in range(1, groups):
            to = (span_of(lax.rem(hi + dh, groups), j, c), t)
            for n, buf in enumerate((kbuf, vbuf)):
                piece = buf.at[h, c, pl.ds(own, g), rows2]
                pltpu.make_async_remote_copy(
                    piece, piece, fwd_sent.at[h, n], fwd_got.at[h, n],
                    device_id=to, device_id_type=pl.DeviceIdType.MESH).start()

    for h in range(hpd):
        relay(h, t)

    def head(h, carry):
        for k in WAITS(toks):
            relay(h, shift_tok(k))
            if k == toks // 2 and h + 1 < hpd:
                issue("kv", h + 1, far)
                issue("q", h + 1, far)
        if groups > 1:
            for n, buf in enumerate((kbuf, vbuf)):
                wait_bytes(buf.at[h, c, pl.ds(0, (groups - 1) * g)], fwd_got.at[h, n])
        for n, buf in enumerate((kbuf, vbuf)):
            half = buf.at[h, c]
            pltpu.make_async_remote_copy(
                half, half, core_sent.at[h, n], core_got.at[h, n],
                device_id=(span_of(hi, j, other), t), device_id_type=pl.DeviceIdType.MESH).start()
        for n, buf in enumerate((kbuf, vbuf)):
            wait_bytes(buf.at[h, other], core_got.at[h, n])

        wait_bytes(qbuf.at[h], got_q.at[h])

        def one(i, carry):
            lax.fori_loop(0, ctok // block, lambda b, x: (unit(h, i, b), x)[1], 0)
            at = cols(t, j, h)
            for k in range(toks):
                t2 = lax.rem(t + toks // 2 + k, toks)
                piece = obuf.at[h, i, pl.ds(pl.multiple_of(t2 * rows, rows), rows)]
                to_self = (t2 == t) & (i == j)

                @pl.when(to_self)
                def _():
                    pltpu.make_async_copy(piece, out_ref.at[:, at], out_got).start()

                @pl.when(jnp.logical_not(to_self))
                def _():
                    pltpu.make_async_remote_copy(
                        piece, out_ref.at[:, at], out_sent, out_got,
                        device_id=(span_of(hi, i, c), t2), device_id_type=pl.DeviceIdType.MESH).start()
            return carry

        return lax.fori_loop(0, g, one, carry)

    for h in range(hpd):
        head(h, 0)
    wait_bytes(out_ref, out_got)
    wait_bytes(total.at[pl.ds(0, len(partners) * hpd * rows)], out_sent)
    wait_bytes(total.at[pl.ds(0, len(partners) * 3 * hpd * rows)], sent)
    if g > 1:
        wait_bytes(maskb.at[pl.ds(0, g - 1)], meta_sem.at[4])
        wait_bytes(levelb.at[pl.ds(0, g - 1)], meta_sem.at[5])
    for h in range(hpd):
        for n, buf in enumerate((kbuf, vbuf)):
            if groups > 1:
                wait_bytes(buf.at[h, c, pl.ds(0, (groups - 1) * g)], fwd_sent.at[h, n])
            wait_bytes(buf.at[h, c], core_sent.at[h, n])


def local(queries, keys, values, levels, retiring, block_mask, gates):
    rows = queries.shape[1]
    spans = lax.axis_size("span")
    toks = lax.axis_size("tok")
    per_tok = HEADS // toks
    g = 2 if per_tok % 2 == 0 and spans % 4 == 0 else 1
    hpd = per_tok // g
    chips = spans // 2
    ctok = rows * toks
    block = min(QUERY_BLOCK, ctok)
    feat = queries.shape[2]
    any_ = pl.BlockSpec(memory_space=pl.ANY)
    bf16, f32 = jnp.bfloat16, jnp.float32
    dma = pltpu.SemaphoreType.DMA
    out = pl.pallas_call(
        functools.partial(kernel, (spans, toks, g, hpd, rows)),
        out_shape=pltpu.VMEM((rows, feat), bf16),
        in_specs=[any_] * 7,
        out_specs=pl.BlockSpec(memory_space=pltpu.VMEM),
        scratch_shapes=[
            pltpu.VMEM((hpd, g, ctok, HEAD_DIM), bf16),
            pltpu.VMEM((hpd, 2, chips, ctok, HEAD_DIM), bf16),
            pltpu.VMEM((hpd, 2, chips, ctok, HEAD_DIM), bf16),
            pltpu.VMEM((g, 1, spans), jnp.int32),
            pltpu.VMEM((g, 1, 1), jnp.int32),
            pltpu.VMEM((1, 1), jnp.int32),
            pltpu.VMEM((gates.shape[0], hpd * HEAD_DIM), f32),
            pltpu.VMEM((g, 8, hpd * HEAD_DIM), f32),
            pltpu.VMEM((2 * chips, ctok, block), f32),
            pltpu.VMEM((hpd, g, ctok, HEAD_DIM), bf16),
            pltpu.VMEM(((toks * g - 1) * 3 * hpd * rows, HEAD_DIM), bf16),
            dma, dma((hpd, toks)), dma((hpd,)), dma((6,)),
            dma((hpd, 2)), dma((hpd, 2)), dma((hpd, 2)), dma((hpd, 2)),
            dma, dma,
        ],
        compiler_params=pltpu.CompilerParams(
            collective_id=0, has_side_effects=True, vmem_limit_bytes=60000000),
    )(queries[0], keys[0], values[0], block_mask, levels[None], retiring[None], gates)
    return out[None]


def solution(mesh):
    return jax.shard_map(
        local,
        mesh=mesh,
        in_specs=(
            P("span", "tok", None),
            P("span", "tok", None),
            P("span", "tok", None),
            P("span"),
            P(),
            P("span", None),
            P(),
        ),
        out_specs=P("span", "tok", None),
        check_vma=False,
    )
```

```python
import functools

import jax
import jax.numpy as jnp
from jax import lax
from jax.experimental import pallas as pl
from jax.experimental.pallas import tpu as pltpu
from jax.sharding import PartitionSpec as P

HEADS = 24
HEAD_DIM = 128
QUERY_BLOCK = 256
UNROLLED_KEYS = 2048


def plan(hpd, toks, g):
    half = toks // 2
    cross, side, near, every = range(half, toks), range(1, half), (0,), range(toks)
    steps = []
    for h in range(hpd):
        steps += [("keep", "kv", h), ("keep", "q", h)]
    rest = [("kv", h) for h in range(1, hpd)] + [("q", h) for h in range(1, hpd)]
    for kind in ("kv", "q"):
        steps += [("send", kind, 0, cross), ("send", kind, 0, side), ("send", kind, 0, near)]
    for kind, h in rest:
        steps += [("inner", kind, h, cross), ("inner", kind, h, side), ("inner", kind, h, near)]
    steps += ["meta"]
    for k in range(toks):
        steps += [("relay", 0, k)]
        if k:
            steps += [("swap", 0, k - 1)]
    for kind, h in rest:
        steps += [("outer", kind, h, cross), ("outer", kind, h, side), ("outer", kind, h, near)]
    steps += [("relay", h, 0) for h in range(1, hpd)] + [("swap", h, 0) for h in range(1, hpd)]
    steps += [("swap", 0, toks - 1), ("ready", 0), ("queried", 0)]
    steps += [("mixed", 0, 0), ("give", 0, 0)]
    for h in range(1, hpd):
        for k in range(1, toks - 1):
            steps += [("relay", h, k)]
    for i in range(1, g):
        steps += [("mixed", 0, i), ("give", 0, i)]
    steps += [("relay", h, toks - 1) for h in range(1, hpd)]
    for h in range(1, hpd):
        steps += [("swap", h, k) for k in range(1, toks)]
        steps += [("ready", h), ("queried", h)]
        for i in range(g):
            steps += [("mixed", h, i), ("give", h, i)]
    return steps

def kernel(dims, q_ref, k_ref, v_ref, mask_ref, level_ref, retiring_ref, gates_ref, out_ref,
           qbuf, kbuf, vbuf, maskb, levelb, retb, gateb, mbuf, sbuf, obuf, total,
           sent, got, got_q, meta_sem, fwd_sent, fwd_got, core_sent, core_got, out_sent, out_got):
    spans, toks, g, hpd, rows = dims
    chips = spans // 2
    groups = chips // g
    ctok = rows * toks
    d = HEAD_DIM
    s = lax.axis_index("span")
    t = lax.axis_index("tok")
    c = lax.rem(s, 2)
    p = lax.div(s, 2)
    j = lax.rem(p, g)
    hi = lax.div(p, g)
    own = hi * g
    other = 1 - c

    def span_of(hi_, j_, c_):
        return (hi_ * g + j_) * 2 + c_

    half = toks // 2

    def place(k):
        if toks % 2:
            return lax.rem(t + k, toks)
        side = lax.div(t, half)
        if k < half:
            return side * half + lax.rem(t + k, half)
        return (1 - side) * (toks - 1 - (k - half)) + side * (k - half)

    partners = [(k, dj) for k in range(toks) for dj in range(g) if (k, dj) != (0, 0)]

    def partner(k, dj):
        return place(k), lax.rem(j + dj, g)

    barrier = pltpu.get_barrier_semaphore()
    count = 0
    for dt, dj in partners:
        t2, j2 = partner(dt, dj)
        pl.semaphore_signal(barrier, inc=1, device_id=(span_of(hi, j2, c), t2),
                            device_id_type=pl.DeviceIdType.MESH)
        count += 1
    for dh in range(1, groups):
        pl.semaphore_signal(barrier, inc=1, device_id=(span_of(lax.rem(hi + dh, groups), j, c), t),
                            device_id_type=pl.DeviceIdType.MESH)
        count += 1
    pl.semaphore_signal(barrier, inc=1, device_id=(span_of(hi, j, other), t),
                        device_id_type=pl.DeviceIdType.MESH)
    pl.semaphore_wait(barrier, count + 1)

    def cols(t_, j_, h):
        return pl.ds(pl.multiple_of(((t_ * g + j_) * hpd + h) * d, d), d)

    my_rows = pl.ds(pl.multiple_of(t * rows, rows), rows)

    def arrays(kind, h):
        if kind == "q":
            return ((q_ref, qbuf.at[h, j, my_rows]),), got_q.at[h]
        return ((k_ref, kbuf.at[h, c, p, my_rows]), (v_ref, vbuf.at[h, c, p, my_rows])), got.at[h, t]

    def issue(kind, h, which):
        pairs, arrive = arrays(kind, h)
        for dt, dj in which:
            t2, j2 = partner(dt, dj)
            for src, dst in pairs:
                pltpu.make_async_remote_copy(
                    src.at[:, cols(t2, j2, h)], dst, sent, arrive,
                    device_id=(span_of(hi, j2, c), t2), device_id_type=pl.DeviceIdType.MESH).start()

    def keep(kind, h):
        pairs, arrive = arrays(kind, h)
        for src, dst in pairs:
            pltpu.make_async_copy(src.at[:, cols(t, j, h)], dst, arrive).start()

    def send(kind, h, ks):
        issue(kind, h, [a for a in partners if a[0] in ks])

    outer = lax.rem(t + 1, toks) < 2 if toks > 2 else t >= 0

    def send_outer(kind, h, ks):
        @pl.when(outer)
        def _():
            send(kind, h, ks)

    def send_inner(kind, h, ks):
        @pl.when(jnp.logical_not(outer))
        def _():
            send(kind, h, ks)

    sends = {"keep": keep, "send": send, "outer": send_outer, "inner": send_inner}
    steps = plan(hpd, toks, g)
    begin = steps.index("meta")
    for step in steps[:begin]:
        sends[step[0]](*step[1:])

    def wait_bytes(ref, sem):
        pltpu.make_async_copy(ref, ref, sem).wait()

    mine = pl.ds(pl.multiple_of((t * g + j) * hpd * d, d), hpd * d)
    pltpu.make_async_copy(retiring_ref, retb, meta_sem.at[2]).start()
    pltpu.make_async_copy(gates_ref.at[:, mine], gateb, meta_sem.at[3]).start()
    for n, (src, dst) in enumerate(((mask_ref, maskb.at[j]), (level_ref, levelb.at[j]))):
        pltpu.make_async_copy(src, dst, meta_sem.at[n]).start()
        for dj in range(1, g):
            t2, j2 = partner(0, dj)
            pltpu.make_async_remote_copy(
                src, dst, meta_sem.at[4 + n], meta_sem.at[n],
                device_id=(span_of(hi, j2, c), t2), device_id_type=pl.DeviceIdType.MESH).start()
    wait_bytes(retb, meta_sem.at[2])
    wait_bytes(gateb, meta_sem.at[3])
    wait_bytes(maskb, meta_sem.at[0])
    wait_bytes(levelb, meta_sem.at[1])
    lane = lax.broadcasted_iota(jnp.int32, (1, spans), 1)
    level_at = lax.broadcasted_iota(jnp.int32, gateb.shape, 0)

    def age(slot):
        return lax.rem(slot - retb[...] + spans, spans)

    for i in range(g):
        slot = span_of(hi, i, c)
        see = (lane == slot) | ((maskb[i] == 1) & (age(lane) < age(slot)))
        mbuf[i, 1:2, 0:spans] = jnp.where(see, 1.0, 0.0)
        mbuf[i, 0:1] = jnp.sum(jnp.where(level_at == levelb[i], gateb[...], 0.0), axis=0, keepdims=True)
    c2 = jnp.float32(HEAD_DIM ** -0.5 * 1.4426950408889634)
    unrolled = 2 * chips * ctok <= UNROLLED_KEYS
    block = min(QUERY_BLOCK, ctok)

    def loop(count, body, carry):
        if unrolled:
            for n in range(count):
                carry = body(n, carry)
            return carry
        return lax.fori_loop(0, count, body, carry)

    def seen(i, half, chip):
        flags = mbuf[i, 1:2, 0:spans]
        lane = lax.broadcasted_iota(jnp.int32, flags.shape, 1)
        hit = lane == chip * 2 + half
        return jnp.sum(jnp.where(hit, flags, 0.0), axis=1, keepdims=True) > 0.5

    def scores(h, i, at, half, slot0, top):
        query = qbuf[h, i, at]

        def body(chip, top):
            score = lax.dot_general(kbuf[h, half, chip], query, (((1,), (1,)), ((), ())),
                                    preferred_element_type=jnp.float32)
            sbuf[slot0 + chip] = score
            best = jnp.max(score, axis=0, keepdims=True)
            return jnp.maximum(top, jnp.where(seen(i, half, chip), best, -1e30))

        return loop(chips, body, top)

    def mix(h, i, half, slot0, shift, carry):
        def body(chip, carry):
            acc, norm = carry
            minus = jnp.where(seen(i, half, chip), shift, 1e30)
            weight = jnp.exp2(sbuf[slot0 + chip] * c2 - minus)
            norm = norm + jnp.sum(weight, axis=0, keepdims=True)
            acc = acc + lax.dot_general(vbuf[h, half, chip], weight.astype(jnp.bfloat16),
                                        (((0,), (0,)), ((), ())), preferred_element_type=jnp.float32)
            return acc, norm

        return loop(chips, body, carry)

    def unit(h, i, b):
        at = pl.ds(b * block, block)
        top = jnp.full((1, block), -1e30, jnp.float32)
        top = scores(h, i, at, c, 0, top)
        top = scores(h, i, at, other, chips, top)
        shift = top * c2
        carry = (jnp.zeros((d, block), jnp.float32), jnp.zeros((1, block), jnp.float32))
        carry = mix(h, i, c, 0, shift, carry)
        acc, norm = mix(h, i, other, chips, shift, carry)
        mixed = (acc / norm).T
        gate = mbuf[i, 0:1, pl.ds(pl.multiple_of(h * d, d), d)]
        obuf[h, i, at] = (mixed * gate).astype(jnp.bfloat16)

    def forward(h, t2, first, many, to, sem, arrive):
        rows2 = pl.ds(pl.multiple_of(t2 * rows, rows), rows)
        for buf in (kbuf, vbuf):
            piece = buf.at[h, c, pl.ds(first, many), rows2]
            pltpu.make_async_remote_copy(
                piece, piece, sem, arrive, device_id=to, device_id_type=pl.DeviceIdType.MESH).start()

    def relay(h, k):
        t2 = place(k)
        wait_bytes(total.at[pl.ds(0, 2 * g * rows)], got.at[h, t2])
        for dh in range(1, groups):
            forward(h, t2, own, g, (span_of(lax.rem(hi + dh, groups), j, c), t), fwd_sent, fwd_got.at[h, t2])
        forward(h, t2, own, g, (span_of(hi, j, other), t), core_sent, core_got.at[h])

    def swap(h, k):
        t2 = place(k)
        if groups > 1:
            wait_bytes(total.at[pl.ds(0, 2 * (groups - 1) * g * rows)], fwd_got.at[h, t2])
        for dh in range(1, groups):
            forward(h, t2, lax.rem(hi + dh, groups) * g, g, (span_of(hi, j, other), t), core_sent, core_got.at[h])

    def ready(h):
        both = pl.ds(0, 2)
        wait_bytes(kbuf.at[h, both, pl.ds(0, chips)], core_got.at[h])

    def queried(h):
        wait_bytes(qbuf.at[h], got_q.at[h])

    def mixed(h, i):
        for b in range(ctok // block):
            unit(h, i, b)

    def give(h, i):
        at = cols(t, j, h)
        for k in reversed(range(toks)):
            t2 = place(k)
            piece = obuf.at[h, i, pl.ds(pl.multiple_of(t2 * rows, rows), rows)]

            def remote():
                pltpu.make_async_remote_copy(
                    piece, out_ref.at[:, at], out_sent, out_got,
                    device_id=(span_of(hi, i, c), t2), device_id_type=pl.DeviceIdType.MESH).start()

            if k:
                remote()
                continue

            @pl.when(i == j)
            def _():
                pltpu.make_async_copy(piece, out_ref.at[:, at], out_got).start()

            @pl.when(i != j)
            def _():
                remote()

    ops = {**sends, "relay": relay, "swap": swap, "ready": ready, "queried": queried,
           "mixed": mixed, "give": give}
    for step in steps[begin + 1:]:
        ops[step[0]](*step[1:])
    wait_bytes(out_ref, out_got)
    wait_bytes(total.at[pl.ds(0, len(partners) * hpd * rows)], out_sent)
    wait_bytes(total.at[pl.ds(0, len(partners) * 3 * hpd * rows)], sent)
    if g > 1:
        wait_bytes(maskb.at[pl.ds(0, g - 1)], meta_sem.at[4])
        wait_bytes(levelb.at[pl.ds(0, g - 1)], meta_sem.at[5])
    for h in range(hpd):
        for n, buf in enumerate((kbuf, vbuf)):
            if groups > 1:
                wait_bytes(buf.at[h, c, pl.ds(0, (groups - 1) * g)], fwd_sent)
            wait_bytes(buf.at[h, c], core_sent)


def local(queries, keys, values, levels, retiring, block_mask, gates):
    rows = queries.shape[1]
    spans = lax.axis_size("span")
    toks = lax.axis_size("tok")
    per_tok = HEADS // toks
    g = 2 if per_tok % 2 == 0 and spans % 4 == 0 else 1
    hpd = per_tok // g
    chips = spans // 2
    ctok = rows * toks
    block = min(QUERY_BLOCK, ctok)
    feat = queries.shape[2]
    any_ = pl.BlockSpec(memory_space=pl.ANY)
    bf16, f32 = jnp.bfloat16, jnp.float32
    dma = pltpu.SemaphoreType.DMA
    out = pl.pallas_call(
        functools.partial(kernel, (spans, toks, g, hpd, rows)),
        out_shape=pltpu.VMEM((rows, feat), bf16),
        in_specs=[any_] * 7,
        out_specs=pl.BlockSpec(memory_space=pltpu.VMEM),
        scratch_shapes=[
            pltpu.VMEM((hpd, g, ctok, HEAD_DIM), bf16),
            pltpu.VMEM((hpd, 2, chips, ctok, HEAD_DIM), bf16),
            pltpu.VMEM((hpd, 2, chips, ctok, HEAD_DIM), bf16),
            pltpu.VMEM((g, 1, spans), jnp.int32),
            pltpu.VMEM((g, 1, 1), jnp.int32),
            pltpu.VMEM((1, 1), jnp.int32),
            pltpu.VMEM((gates.shape[0], hpd * HEAD_DIM), f32),
            pltpu.VMEM((g, 8, hpd * HEAD_DIM), f32),
            pltpu.VMEM((2 * chips, ctok, block), f32),
            pltpu.VMEM((hpd, g, ctok, HEAD_DIM), bf16),
            pltpu.VMEM(((toks * g - 1) * 3 * hpd * rows, HEAD_DIM), bf16),
            dma, dma((hpd, toks)), dma((hpd,)), dma((6,)),
            dma, dma((hpd, toks)), dma, dma((hpd,)),
            dma, dma,
        ],
        compiler_params=pltpu.CompilerParams(
            collective_id=0, has_side_effects=True, vmem_limit_bytes=60000000),
    )(queries[0], keys[0], values[0], block_mask, levels[None], retiring[None], gates)
    return out[None]


def solution(mesh):
    return jax.shard_map(
        local,
        mesh=mesh,
        in_specs=(
            P("span", "tok", None),
            P("span", "tok", None),
            P("span", "tok", None),
            P("span"),
            P(),
            P("span", None),
            P(),
        ),
        out_specs=P("span", "tok", None),
        check_vma=False,
    )
```

```python
import functools

import jax
import jax.numpy as jnp
from jax import lax
from jax.experimental import pallas as pl
from jax.experimental.pallas import tpu as pltpu
from jax.sharding import PartitionSpec as P

HEADS = 24
HEAD_DIM = 128
QUERY_BLOCK = 256
UNROLLED_KEYS = 2048


def plan(hpd, toks, g):
    half = toks // 2
    cross, side, near, every = range(half, toks), range(1, half), (0,), range(toks)
    steps = []
    for h in range(hpd):
        steps += [("keep", "kv", h), ("keep", "q", h)]
    kinds = [("kv", h) for h in range(hpd)]
    qs = [("q", h) for h in range(hpd)]
    for kind in kinds:
        steps += [("send", *kind, part) for part in (cross, side, near)]
    for kind in qs:
        steps += [("inner", *kind, part) for part in (cross, side, near)]
    steps += ["meta"]
    arrivals = [(h, 0) for h in range(hpd)] + [(h, k) for h in range(hpd) for k in range(1, toks)]
    lag, pending = 3, []
    for n, (h, k) in enumerate(arrivals):
        steps += [("relay", h, k)]
        pending += [(h, k)]
        if len(pending) > lag:
            steps += [("swap", *pending.pop(0))]
        if (h, k) == (hpd - 1, toks - 1):
            steps += [("outer", *kind, part) for kind in qs for part in (cross, side, near)]
    for h in range(hpd):
        steps += [("swap", *a) for a in pending if a[0] == h] + [("ready", h), ("queried", h)]
        for i in range(g):
            steps += [("mixed", h, i), ("give", h, i)]
    return steps

def kernel(dims, q_ref, k_ref, v_ref, mask_ref, level_ref, retiring_ref, gates_ref, out_ref,
           qbuf, kbuf, vbuf, maskb, levelb, retb, gateb, mbuf, sbuf, obuf, total,
           sent, got, got_q, meta_sem, fwd_sent, fwd_got, core_sent, core_got, out_sent, out_got):
    spans, toks, g, hpd, rows = dims
    chips = spans // 2
    groups = chips // g
    ctok = rows * toks
    d = HEAD_DIM
    s = lax.axis_index("span")
    t = lax.axis_index("tok")
    c = lax.rem(s, 2)
    p = lax.div(s, 2)
    j = lax.rem(p, g)
    hi = lax.div(p, g)
    own = hi * g
    other = 1 - c

    def span_of(hi_, j_, c_):
        return (hi_ * g + j_) * 2 + c_

    half = toks // 2

    def place(k):
        if toks % 2:
            return lax.rem(t + k, toks)
        side = lax.div(t, half)
        if k < half:
            return side * half + lax.rem(t + k, half)
        return (1 - side) * (toks - 1 - (k - half)) + side * (k - half)

    partners = [(k, dj) for k in range(toks) for dj in range(g) if (k, dj) != (0, 0)]

    def partner(k, dj):
        return place(k), lax.rem(j + dj, g)

    barrier = pltpu.get_barrier_semaphore()
    count = 0
    for dt, dj in partners:
        t2, j2 = partner(dt, dj)
        pl.semaphore_signal(barrier, inc=1, device_id=(span_of(hi, j2, c), t2),
                            device_id_type=pl.DeviceIdType.MESH)
        count += 1
    for dh in range(1, groups):
        pl.semaphore_signal(barrier, inc=1, device_id=(span_of(lax.rem(hi + dh, groups), j, c), t),
                            device_id_type=pl.DeviceIdType.MESH)
        count += 1
    pl.semaphore_signal(barrier, inc=1, device_id=(span_of(hi, j, other), t),
                        device_id_type=pl.DeviceIdType.MESH)
    pl.semaphore_wait(barrier, count + 1)

    def cols(t_, j_, h):
        return pl.ds(pl.multiple_of(((t_ * g + j_) * hpd + h) * d, d), d)

    my_rows = pl.ds(pl.multiple_of(t * rows, rows), rows)

    def arrays(kind, h):
        if kind == "q":
            return ((q_ref, qbuf.at[h, j, my_rows]),), got_q.at[h]
        return ((k_ref, kbuf.at[h, c, p, my_rows]), (v_ref, vbuf.at[h, c, p, my_rows])), got.at[h, t]

    def issue(kind, h, which):
        pairs, arrive = arrays(kind, h)
        for dt, dj in which:
            t2, j2 = partner(dt, dj)
            for src, dst in pairs:
                pltpu.make_async_remote_copy(
                    src.at[:, cols(t2, j2, h)], dst, sent, arrive,
                    device_id=(span_of(hi, j2, c), t2), device_id_type=pl.DeviceIdType.MESH).start()

    def keep(kind, h):
        pairs, arrive = arrays(kind, h)
        for src, dst in pairs:
            pltpu.make_async_copy(src.at[:, cols(t, j, h)], dst, arrive).start()

    def send(kind, h, ks):
        issue(kind, h, [a for a in partners if a[0] in ks])

    outer = lax.rem(t + 1, toks) < 2 if toks > 2 else t >= 0

    def send_outer(kind, h, ks):
        @pl.when(outer)
        def _():
            send(kind, h, ks)

    def send_inner(kind, h, ks):
        @pl.when(jnp.logical_not(outer))
        def _():
            send(kind, h, ks)

    sends = {"keep": keep, "send": send, "outer": send_outer, "inner": send_inner}
    steps = plan(hpd, toks, g)
    begin = steps.index("meta")
    for step in steps[:begin]:
        sends[step[0]](*step[1:])

    def wait_bytes(ref, sem):
        pltpu.make_async_copy(ref, ref, sem).wait()

    mine = pl.ds(pl.multiple_of((t * g + j) * hpd * d, d), hpd * d)
    pltpu.make_async_copy(retiring_ref, retb, meta_sem.at[2]).start()
    pltpu.make_async_copy(gates_ref.at[:, mine], gateb, meta_sem.at[3]).start()
    for n, (src, dst) in enumerate(((mask_ref, maskb.at[j]), (level_ref, levelb.at[j]))):
        pltpu.make_async_copy(src, dst, meta_sem.at[n]).start()
        for dj in range(1, g):
            t2, j2 = partner(0, dj)
            pltpu.make_async_remote_copy(
                src, dst, meta_sem.at[4 + n], meta_sem.at[n],
                device_id=(span_of(hi, j2, c), t2), device_id_type=pl.DeviceIdType.MESH).start()
    wait_bytes(retb, meta_sem.at[2])
    wait_bytes(gateb, meta_sem.at[3])
    wait_bytes(maskb, meta_sem.at[0])
    wait_bytes(levelb, meta_sem.at[1])
    lane = lax.broadcasted_iota(jnp.int32, (1, spans), 1)
    level_at = lax.broadcasted_iota(jnp.int32, gateb.shape, 0)

    def age(slot):
        return lax.rem(slot - retb[...] + spans, spans)

    for i in range(g):
        slot = span_of(hi, i, c)
        see = (lane == slot) | ((maskb[i] == 1) & (age(lane) < age(slot)))
        mbuf[i, 1:2, 0:spans] = jnp.where(see, 1.0, 0.0)
        mbuf[i, 0:1] = jnp.sum(jnp.where(level_at == levelb[i], gateb[...], 0.0), axis=0, keepdims=True)
    c2 = jnp.float32(HEAD_DIM ** -0.5 * 1.4426950408889634)
    unrolled = 2 * chips * ctok <= UNROLLED_KEYS
    block = min(QUERY_BLOCK, ctok)

    def loop(count, body, carry):
        if unrolled:
            for n in range(count):
                carry = body(n, carry)
            return carry
        return lax.fori_loop(0, count, body, carry)

    def seen(i, half, chip):
        flags = mbuf[i, 1:2, 0:spans]
        lane = lax.broadcasted_iota(jnp.int32, flags.shape, 1)
        hit = lane == chip * 2 + half
        return jnp.sum(jnp.where(hit, flags, 0.0), axis=1, keepdims=True) > 0.5

    def scores(h, i, at, half, slot0, top):
        query = qbuf[h, i, at]

        def body(chip, top):
            score = lax.dot_general(kbuf[h, half, chip], query, (((1,), (1,)), ((), ())),
                                    preferred_element_type=jnp.float32)
            sbuf[slot0 + chip] = score
            best = jnp.max(score, axis=0, keepdims=True)
            return jnp.maximum(top, jnp.where(seen(i, half, chip), best, -1e30))

        return loop(chips, body, top)

    def mix(h, i, half, slot0, shift, carry):
        def body(chip, carry):
            acc, norm = carry
            minus = jnp.where(seen(i, half, chip), shift, 1e30)
            weight = jnp.exp2(sbuf[slot0 + chip] * c2 - minus)
            norm = norm + jnp.sum(weight, axis=0, keepdims=True)
            acc = acc + lax.dot_general(vbuf[h, half, chip], weight.astype(jnp.bfloat16),
                                        (((0,), (0,)), ((), ())), preferred_element_type=jnp.float32)
            return acc, norm

        return loop(chips, body, carry)

    def unit(h, i, b):
        at = pl.ds(b * block, block)
        top = jnp.full((1, block), -1e30, jnp.float32)
        top = scores(h, i, at, c, 0, top)
        top = scores(h, i, at, other, chips, top)
        shift = top * c2
        carry = (jnp.zeros((d, block), jnp.float32), jnp.zeros((1, block), jnp.float32))
        carry = mix(h, i, c, 0, shift, carry)
        acc, norm = mix(h, i, other, chips, shift, carry)
        mixed = (acc / norm).T
        gate = mbuf[i, 0:1, pl.ds(pl.multiple_of(h * d, d), d)]
        obuf[h, i, at] = (mixed * gate).astype(jnp.bfloat16)

    def forward(h, t2, first, many, to, sem, arrive):
        rows2 = pl.ds(pl.multiple_of(t2 * rows, rows), rows)
        for buf in (kbuf, vbuf):
            piece = buf.at[h, c, pl.ds(first, many), rows2]
            pltpu.make_async_remote_copy(
                piece, piece, sem, arrive, device_id=to, device_id_type=pl.DeviceIdType.MESH).start()

    def relay(h, k):
        t2 = place(k)
        wait_bytes(total.at[pl.ds(0, 2 * g * rows)], got.at[h, t2])
        for dh in range(1, groups):
            forward(h, t2, own, g, (span_of(lax.rem(hi + dh, groups), j, c), t), fwd_sent, fwd_got.at[h, t2])
        forward(h, t2, own, g, (span_of(hi, j, other), t), core_sent, core_got.at[h])

    def swap(h, k):
        t2 = place(k)
        if groups > 1:
            wait_bytes(total.at[pl.ds(0, 2 * (groups - 1) * g * rows)], fwd_got.at[h, t2])
        for dh in range(1, groups):
            forward(h, t2, lax.rem(hi + dh, groups) * g, g, (span_of(hi, j, other), t), core_sent, core_got.at[h])

    def ready(h):
        both = pl.ds(0, 2)
        wait_bytes(kbuf.at[h, both, pl.ds(0, chips)], core_got.at[h])

    def queried(h):
        wait_bytes(qbuf.at[h], got_q.at[h])

    def mixed(h, i):
        for b in range(ctok // block):
            unit(h, i, b)

    def give(h, i):
        at = cols(t, j, h)
        for k in reversed(range(toks)):
            t2 = place(k)
            piece = obuf.at[h, i, pl.ds(pl.multiple_of(t2 * rows, rows), rows)]

            def remote():
                pltpu.make_async_remote_copy(
                    piece, out_ref.at[:, at], out_sent, out_got,
                    device_id=(span_of(hi, i, c), t2), device_id_type=pl.DeviceIdType.MESH).start()

            if k:
                remote()
                continue

            @pl.when(i == j)
            def _():
                pltpu.make_async_copy(piece, out_ref.at[:, at], out_got).start()

            @pl.when(i != j)
            def _():
                remote()

    ops = {**sends, "relay": relay, "swap": swap, "ready": ready, "queried": queried,
           "mixed": mixed, "give": give}
    for step in steps[begin + 1:]:
        ops[step[0]](*step[1:])
    wait_bytes(out_ref, out_got)
    wait_bytes(total.at[pl.ds(0, len(partners) * hpd * rows)], out_sent)
    wait_bytes(total.at[pl.ds(0, len(partners) * 3 * hpd * rows)], sent)
    if g > 1:
        wait_bytes(maskb.at[pl.ds(0, g - 1)], meta_sem.at[4])
        wait_bytes(levelb.at[pl.ds(0, g - 1)], meta_sem.at[5])
    for h in range(hpd):
        for n, buf in enumerate((kbuf, vbuf)):
            if groups > 1:
                wait_bytes(buf.at[h, c, pl.ds(0, (groups - 1) * g)], fwd_sent)
            wait_bytes(buf.at[h, c], core_sent)


def local(queries, keys, values, levels, retiring, block_mask, gates):
    rows = queries.shape[1]
    spans = lax.axis_size("span")
    toks = lax.axis_size("tok")
    per_tok = HEADS // toks
    g = 2 if per_tok % 2 == 0 and spans % 4 == 0 else 1
    hpd = per_tok // g
    chips = spans // 2
    ctok = rows * toks
    block = min(QUERY_BLOCK, ctok)
    feat = queries.shape[2]
    any_ = pl.BlockSpec(memory_space=pl.ANY)
    bf16, f32 = jnp.bfloat16, jnp.float32
    dma = pltpu.SemaphoreType.DMA
    out = pl.pallas_call(
        functools.partial(kernel, (spans, toks, g, hpd, rows)),
        out_shape=pltpu.VMEM((rows, feat), bf16),
        in_specs=[any_] * 7,
        out_specs=pl.BlockSpec(memory_space=pltpu.VMEM),
        scratch_shapes=[
            pltpu.VMEM((hpd, g, ctok, HEAD_DIM), bf16),
            pltpu.VMEM((hpd, 2, chips, ctok, HEAD_DIM), bf16),
            pltpu.VMEM((hpd, 2, chips, ctok, HEAD_DIM), bf16),
            pltpu.VMEM((g, 1, spans), jnp.int32),
            pltpu.VMEM((g, 1, 1), jnp.int32),
            pltpu.VMEM((1, 1), jnp.int32),
            pltpu.VMEM((gates.shape[0], hpd * HEAD_DIM), f32),
            pltpu.VMEM((g, 8, hpd * HEAD_DIM), f32),
            pltpu.VMEM((2 * chips, ctok, block), f32),
            pltpu.VMEM((hpd, g, ctok, HEAD_DIM), bf16),
            pltpu.VMEM(((toks * g - 1) * 3 * hpd * rows, HEAD_DIM), bf16),
            dma, dma((hpd, toks)), dma((hpd,)), dma((6,)),
            dma, dma((hpd, toks)), dma, dma((hpd,)),
            dma, dma,
        ],
        compiler_params=pltpu.CompilerParams(
            collective_id=0, has_side_effects=True, vmem_limit_bytes=60000000),
    )(queries[0], keys[0], values[0], block_mask, levels[None], retiring[None], gates)
    return out[None]


def solution(mesh):
    return jax.shard_map(
        local,
        mesh=mesh,
        in_specs=(
            P("span", "tok", None),
            P("span", "tok", None),
            P("span", "tok", None),
            P("span"),
            P(),
            P("span", None),
            P(),
        ),
        out_specs=P("span", "tok", None),
        check_vma=False,
    )
```

```python
import functools

import jax
import jax.numpy as jnp
from jax import lax
from jax.experimental import pallas as pl
from jax.experimental.pallas import tpu as pltpu
from jax.sharding import PartitionSpec as P

HEADS = 24
HEAD_DIM = 128
QUERY_BLOCK = 256
UNROLLED_KEYS = 2048


def plan(hpd, toks, g):
    half = toks // 2
    cross, side, near, every = range(half, toks), range(1, half), (0,), range(toks)
    steps = []
    for h in range(hpd):
        steps += [("keep", "kv", h), ("keep", "q", h)]
    kinds = [("kv", h) for h in range(hpd)]
    qs = [("q", h) for h in range(hpd)]
    for kind in kinds:
        steps += [("send", *kind, part) for part in (cross, side, near)]
    for kind in qs:
        steps += [("inner", *kind, part) for part in (cross, side, near)]
    steps += ["meta"]
    arrivals = [(h, 0) for h in range(hpd)] + [(h, k) for h in range(hpd) for k in [*range(half, toks - 1), *range(1, half), toks - 1]]
    lag, pending = 3, []
    for n, (h, k) in enumerate(arrivals):
        steps += [("relay", h, k)]
        pending += [(h, k)]
        if len(pending) > lag:
            steps += [("swap", *pending.pop(0))]
        if (h, k) == (hpd - 1, toks - 1):
            steps += [("outer", *kind, part) for kind in qs for part in (cross, side, near)]
    for h in range(hpd):
        steps += [("swap", *a) for a in pending if a[0] == h] + [("ready", h), ("queried", h)]
        for i in range(g):
            steps += [("mixed", h, i), ("give", h, i)]
    return steps

def kernel(dims, q_ref, k_ref, v_ref, mask_ref, level_ref, retiring_ref, gates_ref, out_ref,
           qbuf, kbuf, vbuf, maskb, levelb, retb, gateb, mbuf, sbuf, obuf, total,
           sent, got, got_q, meta_sem, fwd_sent, fwd_got, core_sent, core_got, out_sent, out_got):
    spans, toks, g, hpd, rows = dims
    chips = spans // 2
    groups = chips // g
    ctok = rows * toks
    d = HEAD_DIM
    s = lax.axis_index("span")
    t = lax.axis_index("tok")
    c = lax.rem(s, 2)
    p = lax.div(s, 2)
    j = lax.rem(p, g)
    hi = lax.div(p, g)
    own = hi * g
    other = 1 - c

    def span_of(hi_, j_, c_):
        return (hi_ * g + j_) * 2 + c_

    half = toks // 2

    def place(k):
        if toks % 2:
            return lax.rem(t + k, toks)
        side = lax.div(t, half)
        if k < half:
            return side * half + lax.rem(t + k, half)
        return (1 - side) * (toks - 1 - (k - half)) + side * (k - half)

    partners = [(k, dj) for k in range(toks) for dj in range(g) if (k, dj) != (0, 0)]

    def partner(k, dj):
        return place(k), lax.rem(j + dj, g)

    barrier = pltpu.get_barrier_semaphore()
    count = 0
    for dt, dj in partners:
        t2, j2 = partner(dt, dj)
        pl.semaphore_signal(barrier, inc=1, device_id=(span_of(hi, j2, c), t2),
                            device_id_type=pl.DeviceIdType.MESH)
        count += 1
    for dh in range(1, groups):
        pl.semaphore_signal(barrier, inc=1, device_id=(span_of(lax.rem(hi + dh, groups), j, c), t),
                            device_id_type=pl.DeviceIdType.MESH)
        count += 1
    pl.semaphore_signal(barrier, inc=1, device_id=(span_of(hi, j, other), t),
                        device_id_type=pl.DeviceIdType.MESH)
    pl.semaphore_wait(barrier, count + 1)

    def cols(t_, j_, h):
        return pl.ds(pl.multiple_of(((t_ * g + j_) * hpd + h) * d, d), d)

    my_rows = pl.ds(pl.multiple_of(t * rows, rows), rows)

    def arrays(kind, h):
        if kind == "q":
            return ((q_ref, qbuf.at[h, j, my_rows]),), got_q.at[h]
        return ((k_ref, kbuf.at[h, c, p, my_rows]), (v_ref, vbuf.at[h, c, p, my_rows])), got.at[h, t]

    def issue(kind, h, which):
        pairs, arrive = arrays(kind, h)
        for dt, dj in which:
            t2, j2 = partner(dt, dj)
            for src, dst in pairs:
                pltpu.make_async_remote_copy(
                    src.at[:, cols(t2, j2, h)], dst, sent, arrive,
                    device_id=(span_of(hi, j2, c), t2), device_id_type=pl.DeviceIdType.MESH).start()

    def keep(kind, h):
        pairs, arrive = arrays(kind, h)
        for src, dst in pairs:
            pltpu.make_async_copy(src.at[:, cols(t, j, h)], dst, arrive).start()

    def send(kind, h, ks):
        issue(kind, h, [a for a in partners if a[0] in ks])

    outer = lax.rem(t + 1, toks) < 2 if toks > 2 else t >= 0

    def send_outer(kind, h, ks):
        @pl.when(outer)
        def _():
            send(kind, h, ks)

    def send_inner(kind, h, ks):
        @pl.when(jnp.logical_not(outer))
        def _():
            send(kind, h, ks)

    sends = {"keep": keep, "send": send, "outer": send_outer, "inner": send_inner}
    steps = plan(hpd, toks, g)
    begin = steps.index("meta")
    for step in steps[:begin]:
        sends[step[0]](*step[1:])

    def wait_bytes(ref, sem):
        pltpu.make_async_copy(ref, ref, sem).wait()

    mine = pl.ds(pl.multiple_of((t * g + j) * hpd * d, d), hpd * d)
    pltpu.make_async_copy(retiring_ref, retb, meta_sem.at[2]).start()
    pltpu.make_async_copy(gates_ref.at[:, mine], gateb, meta_sem.at[3]).start()
    for n, (src, dst) in enumerate(((mask_ref, maskb.at[j]), (level_ref, levelb.at[j]))):
        pltpu.make_async_copy(src, dst, meta_sem.at[n]).start()
        for dj in range(1, g):
            t2, j2 = partner(0, dj)
            pltpu.make_async_remote_copy(
                src, dst, meta_sem.at[4 + n], meta_sem.at[n],
                device_id=(span_of(hi, j2, c), t2), device_id_type=pl.DeviceIdType.MESH).start()
    wait_bytes(retb, meta_sem.at[2])
    wait_bytes(gateb, meta_sem.at[3])
    wait_bytes(maskb, meta_sem.at[0])
    wait_bytes(levelb, meta_sem.at[1])
    lane = lax.broadcasted_iota(jnp.int32, (1, spans), 1)
    level_at = lax.broadcasted_iota(jnp.int32, gateb.shape, 0)

    def age(slot):
        return lax.rem(slot - retb[...] + spans, spans)

    for i in range(g):
        slot = span_of(hi, i, c)
        see = (lane == slot) | ((maskb[i] == 1) & (age(lane) < age(slot)))
        mbuf[i, 1:2, 0:spans] = jnp.where(see, 1.0, 0.0)
        mbuf[i, 0:1] = jnp.sum(jnp.where(level_at == levelb[i], gateb[...], 0.0), axis=0, keepdims=True)
    c2 = jnp.float32(HEAD_DIM ** -0.5 * 1.4426950408889634)
    unrolled = 2 * chips * ctok <= UNROLLED_KEYS
    block = min(QUERY_BLOCK, ctok)

    def loop(count, body, carry):
        if unrolled:
            for n in range(count):
                carry = body(n, carry)
            return carry
        return lax.fori_loop(0, count, body, carry)

    def seen(i, half, chip):
        flags = mbuf[i, 1:2, 0:spans]
        lane = lax.broadcasted_iota(jnp.int32, flags.shape, 1)
        hit = lane == chip * 2 + half
        return jnp.sum(jnp.where(hit, flags, 0.0), axis=1, keepdims=True) > 0.5

    def scores(h, i, at, half, slot0, top):
        query = qbuf[h, i, at]

        def body(chip, top):
            score = lax.dot_general(kbuf[h, half, chip], query, (((1,), (1,)), ((), ())),
                                    preferred_element_type=jnp.float32)
            sbuf[slot0 + chip] = score
            best = jnp.max(score, axis=0, keepdims=True)
            return jnp.maximum(top, jnp.where(seen(i, half, chip), best, -1e30))

        return loop(chips, body, top)

    def mix(h, i, half, slot0, shift, carry):
        def body(chip, carry):
            acc, norm = carry
            minus = jnp.where(seen(i, half, chip), shift, 1e30)
            weight = jnp.exp2(sbuf[slot0 + chip] * c2 - minus)
            norm = norm + jnp.sum(weight, axis=0, keepdims=True)
            acc = acc + lax.dot_general(vbuf[h, half, chip], weight.astype(jnp.bfloat16),
                                        (((0,), (0,)), ((), ())), preferred_element_type=jnp.float32)
            return acc, norm

        return loop(chips, body, carry)

    def unit(h, i, b):
        at = pl.ds(b * block, block)
        top = jnp.full((1, block), -1e30, jnp.float32)
        top = scores(h, i, at, c, 0, top)
        top = scores(h, i, at, other, chips, top)
        shift = top * c2
        carry = (jnp.zeros((d, block), jnp.float32), jnp.zeros((1, block), jnp.float32))
        carry = mix(h, i, c, 0, shift, carry)
        acc, norm = mix(h, i, other, chips, shift, carry)
        mixed = (acc / norm).T
        gate = mbuf[i, 0:1, pl.ds(pl.multiple_of(h * d, d), d)]
        obuf[h, i, at] = (mixed * gate).astype(jnp.bfloat16)

    def forward(h, t2, first, many, to, sem, arrive):
        rows2 = pl.ds(pl.multiple_of(t2 * rows, rows), rows)
        for buf in (kbuf, vbuf):
            piece = buf.at[h, c, pl.ds(first, many), rows2]
            pltpu.make_async_remote_copy(
                piece, piece, sem, arrive, device_id=to, device_id_type=pl.DeviceIdType.MESH).start()

    def relay(h, k):
        t2 = place(k)
        wait_bytes(total.at[pl.ds(0, 2 * g * rows)], got.at[h, t2])
        for dh in range(1, groups):
            forward(h, t2, own, g, (span_of(lax.rem(hi + dh, groups), j, c), t), fwd_sent, fwd_got.at[h, t2])
        forward(h, t2, own, g, (span_of(hi, j, other), t), core_sent, core_got.at[h])

    def swap(h, k):
        t2 = place(k)
        if groups > 1:
            wait_bytes(total.at[pl.ds(0, 2 * (groups - 1) * g * rows)], fwd_got.at[h, t2])
        for dh in range(1, groups):
            forward(h, t2, lax.rem(hi + dh, groups) * g, g, (span_of(hi, j, other), t), core_sent, core_got.at[h])

    def ready(h):
        both = pl.ds(0, 2)
        wait_bytes(kbuf.at[h, both, pl.ds(0, chips)], core_got.at[h])

    def queried(h):
        wait_bytes(qbuf.at[h], got_q.at[h])

    def mixed(h, i):
        for b in range(ctok // block):
            unit(h, i, b)

    def give(h, i):
        at = cols(t, j, h)
        for k in [*range(half, toks), *reversed(range(half))]:
            t2 = place(k)
            piece = obuf.at[h, i, pl.ds(pl.multiple_of(t2 * rows, rows), rows)]

            def remote():
                pltpu.make_async_remote_copy(
                    piece, out_ref.at[:, at], out_sent, out_got,
                    device_id=(span_of(hi, i, c), t2), device_id_type=pl.DeviceIdType.MESH).start()

            if k:
                remote()
                continue

            @pl.when(i == j)
            def _():
                pltpu.make_async_copy(piece, out_ref.at[:, at], out_got).start()

            @pl.when(i != j)
            def _():
                remote()

    ops = {**sends, "relay": relay, "swap": swap, "ready": ready, "queried": queried,
           "mixed": mixed, "give": give}
    for step in steps[begin + 1:]:
        ops[step[0]](*step[1:])
    wait_bytes(out_ref, out_got)
    wait_bytes(total.at[pl.ds(0, len(partners) * hpd * rows)], out_sent)
    wait_bytes(total.at[pl.ds(0, len(partners) * 3 * hpd * rows)], sent)
    if g > 1:
        wait_bytes(maskb.at[pl.ds(0, g - 1)], meta_sem.at[4])
        wait_bytes(levelb.at[pl.ds(0, g - 1)], meta_sem.at[5])
    for h in range(hpd):
        for n, buf in enumerate((kbuf, vbuf)):
            if groups > 1:
                wait_bytes(buf.at[h, c, pl.ds(0, (groups - 1) * g)], fwd_sent)
            wait_bytes(buf.at[h, c], core_sent)


def local(queries, keys, values, levels, retiring, block_mask, gates):
    rows = queries.shape[1]
    spans = lax.axis_size("span")
    toks = lax.axis_size("tok")
    per_tok = HEADS // toks
    g = 2 if per_tok % 2 == 0 and spans % 4 == 0 else 1
    hpd = per_tok // g
    chips = spans // 2
    ctok = rows * toks
    block = min(QUERY_BLOCK, ctok)
    feat = queries.shape[2]
    any_ = pl.BlockSpec(memory_space=pl.ANY)
    bf16, f32 = jnp.bfloat16, jnp.float32
    dma = pltpu.SemaphoreType.DMA
    out = pl.pallas_call(
        functools.partial(kernel, (spans, toks, g, hpd, rows)),
        out_shape=pltpu.VMEM((rows, feat), bf16),
        in_specs=[any_] * 7,
        out_specs=pl.BlockSpec(memory_space=pltpu.VMEM),
        scratch_shapes=[
            pltpu.VMEM((hpd, g, ctok, HEAD_DIM), bf16),
            pltpu.VMEM((hpd, 2, chips, ctok, HEAD_DIM), bf16),
            pltpu.VMEM((hpd, 2, chips, ctok, HEAD_DIM), bf16),
            pltpu.VMEM((g, 1, spans), jnp.int32),
            pltpu.VMEM((g, 1, 1), jnp.int32),
            pltpu.VMEM((1, 1), jnp.int32),
            pltpu.VMEM((gates.shape[0], hpd * HEAD_DIM), f32),
            pltpu.VMEM((g, 8, hpd * HEAD_DIM), f32),
            pltpu.VMEM((2 * chips, ctok, block), f32),
            pltpu.VMEM((hpd, g, ctok, HEAD_DIM), bf16),
            pltpu.VMEM(((toks * g - 1) * 3 * hpd * rows, HEAD_DIM), bf16),
            dma, dma((hpd, toks)), dma((hpd,)), dma((6,)),
            dma, dma((hpd, toks)), dma, dma((hpd,)),
            dma, dma,
        ],
        compiler_params=pltpu.CompilerParams(
            collective_id=0, has_side_effects=True, vmem_limit_bytes=60000000),
    )(queries[0], keys[0], values[0], block_mask, levels[None], retiring[None], gates)
    return out[None]


def solution(mesh):
    return jax.shard_map(
        local,
        mesh=mesh,
        in_specs=(
            P("span", "tok", None),
            P("span", "tok", None),
            P("span", "tok", None),
            P("span"),
            P(),
            P("span", None),
            P(),
        ),
        out_specs=P("span", "tok", None),
        check_vma=False,
    )
```
